32 devices in a mesh: dp: 16 (over z, y, core), tp: 2 (over x).
Axes of the slice: x: 2, y: 2, z: 4, core: 2. Of those that a mesh axis runs over, the one named last changes fastest.
Arguments:
- activations: bfloat16 [2048, 2304], P('dp'), may hold values from -6 to 6
- out_grads: bfloat16 [2048, 2048], P('dp', 'tp'), may hold values from -6 to 6
- right_prev: float32 [2048, 128], P('tp'), may hold values from -6 to 6
Outputs:
- update: float32 [2304, 2048], P('dp', 'tp')
- residual: bfloat16 [36864, 2048], P('dp', 'tp')
The draws below stay inside these ranges and needn't reach their ends.
All inputs are finite; a program needn't handle non-finite values.
Results may differ from the reference program's by a relative error of at most 0.001.
Values sent between devices are 32-bit elements; how exact they have to be, the bound alone decides.
No kernel may reach another device: no remote copies, remote signals or barrier semaphores. Data moves between devices by JAX's collectives and lax.ppermute only.
A program may use at most 64 MiB of HBM per device.

```python
import jax
import jax.numpy as jnp
from jax import lax

ROWS = 2304
COLS = 2048
RANK = 128
TOK_DEV = 128
TOKENS = 2048


def levels(stream_key, shape, shards, least, top_value):
    def one(dim, shards_of):
        draws = jax.random.uniform(jax.random.fold_in(jax.random.fold_in(stream_key, 6), dim), (shards_of,), jnp.float32, least / len(shards), top_value / len(shards))
        return jnp.repeat(jnp.exp(draws), shape[dim] // shards_of).reshape((-1,) + (1,) * (len(shape) - dim - 1))

    gain = one(*shards[0])
    for cut in shards[1:]:
        gain = gain * one(*cut)
    return gain


def centred(own_key, dims, deviation, bound, split=(), held_as=jnp.bfloat16):
    values = jax.random.normal(own_key, dims, jnp.float32) * deviation
    if len(split) > 0:
        values = levels(own_key, dims, split, -0.22, 0.18) * values
    return jnp.clip(values, min=-bound, max=bound).astype(held_as)


def setup_inputs(seed: int = 0) -> dict:
    seeds = jax.random.split(jax.random.key(seed), 4)
    activations = centred(seeds[0], (TOKENS, ROWS), 1.0, 6.0, ((0, 16),))
    out_grads = centred(seeds[1], (TOKENS, COLS), 1.0, 6.0, ((0, 16), (1, 2)))
    right_prev = centred(seeds[2], (COLS, RANK), 1.0, 6.0, ((0, 2),), jnp.float32)
    return dict(activations=activations, out_grads=out_grads, right_prev=right_prev)


def orthonormal(left_sum):
    gram_matrix = jnp.dot(left_sum.T, left_sum, precision=lax.Precision.HIGHEST)
    ridge = 1e-06 * jnp.trace(gram_matrix) / gram_matrix.shape[0]
    gram_matrix = gram_matrix + ridge * jnp.eye(gram_matrix.shape[0], dtype=gram_matrix.dtype)
    lower = jnp.linalg.cholesky(gram_matrix)
    return jax.scipy.linalg.solve_triangular(lower, left_sum.T, lower=True).T

def reference(activations, out_grads, right_prev):
    replicas = activations.shape[0] // TOK_DEV
    acts_all = activations.reshape(replicas, TOK_DEV, ROWS)
    grads_all = out_grads.reshape(replicas, TOK_DEV, COLS)

    def gradient_of(acts_block, grads_block):
        return jnp.dot(acts_block.T.astype(jnp.float32), grads_block.astype(jnp.float32), preferred_element_type=jnp.float32)

    def left_step(carry, inputs):
        gradient = gradient_of(inputs[0], inputs[1])
        return (carry + jnp.dot(gradient, right_prev, precision=lax.Precision.HIGHEST), None)
    left_sum, _ = lax.scan(left_step, jnp.zeros((ROWS, RANK), jnp.float32), (acts_all, grads_all))
    left_basis = orthonormal(left_sum)

    def right_step(carry, inputs):
        gradient = gradient_of(inputs[0], inputs[1])
        return (carry + jnp.dot(gradient.T, left_basis, precision=lax.Precision.HIGHEST), None)
    right_factor, _ = lax.scan(right_step, jnp.zeros((COLS, RANK), jnp.float32), (acts_all, grads_all))
    right_factor = right_factor / replicas
    update = jnp.dot(left_basis, right_factor.T, precision=lax.Precision.HIGHEST)

    def residual_of(inputs):
        return (gradient_of(inputs[0], inputs[1]) - update).astype(jnp.bfloat16)
    residual = lax.map(residual_of, (acts_all, grads_all)).reshape(replicas * ROWS, COLS)
    return (update, residual)
```

```python
import jax
import jax.numpy as jnp
from jax import lax
from jax.sharding import PartitionSpec as P

HI = lax.Precision.HIGHEST


def factors_of(count):
    found, divisor = [], 2
    while count > 1:
        while count % divisor == 0:
            found.append(divisor)
            count //= divisor
        divisor += 1
    return found


def stages_of(axis):
    stages, stride = [], 1
    for radix in factors_of(lax.axis_size(axis)):
        stages.append((radix, stride))
        stride *= radix
    return stages


def shifted(value, axis, radix, stride, step):
    pairs = []
    for index in range(lax.axis_size(axis)):
        digit = index // stride % radix
        pairs.append((index, index + ((digit + step) % radix - digit) * stride))
    return lax.ppermute(value, axis, pairs)


def all_sum(value, axis):
    for radix, stride in stages_of(axis):
        parts = [shifted(value, axis, radix, stride, step) for step in range(1, radix)]
        for part in parts:
            value = value + part
    return value


def scatter_sum(value, axis):
    position = lax.axis_index(axis)
    for radix, stride in stages_of(axis):
        digit = position // stride % radix
        rows = value.shape[0] // radix
        received = []
        for step in range(1, radix):
            start = (digit + step) % radix * rows
            block = lax.dynamic_slice_in_dim(value, start, rows, 0)
            received.append(shifted(block, axis, radix, stride, step))
        value = lax.dynamic_slice_in_dim(value, digit * rows, rows, 0)
        for block in received:
            value = value + block
    return value


def gather_rows(value, axis):
    position = lax.axis_index(axis)
    for radix, stride in reversed(stages_of(axis)):
        digit = position // stride % radix
        rows = value.shape[0]
        whole = jnp.zeros((radix * rows, value.shape[1]), value.dtype)
        whole = lax.dynamic_update_slice_in_dim(whole, value, digit * rows, 0)
        received = [shifted(value, axis, radix, stride, step) for step in range(1, radix)]
        for step, block in enumerate(received, 1):
            start = (digit + radix - step) % radix * rows
            whole = lax.dynamic_update_slice_in_dim(whole, block, start, 0)
        value = whole
    return value


def bf16_terms(value, count):
    terms = []
    for _ in range(count):
        top = lax.reduce_precision(value, 8, 7)
        terms.append(top.astype(jnp.bfloat16))
        value = value - top
    return terms


def exact_dot(narrow, wide, contract, count=3):
    dims = ((contract[:1], contract[1:]), ((), ()))
    total = None
    for term in reversed(bf16_terms(wide, count)):
        part = lax.dot_general(narrow, term, dims, preferred_element_type=jnp.float32)
        total = part if total is None else total + part
    return total


def padded_rows(value, multiple):
    extra = -value.shape[0] % multiple
    return jnp.pad(value, ((0, extra), (0, 0))) if extra else value


def per_device(activations, out_grads, right_prev):
    replicas, columns = lax.axis_size("dp"), lax.axis_size("tp")
    rows, rank = activations.shape[1], right_prev.shape[1]
    my_rows = rows // columns

    projected = all_sum(exact_dot(out_grads, right_prev, (1, 0)), "tp")
    own = lax.dynamic_slice_in_dim(activations, lax.axis_index("tp") * my_rows, my_rows, 1)
    left_part = padded_rows(exact_dot(own, projected, (0, 0)), replicas)
    left_own = gather_rows(scatter_sum(left_part, "dp"), "dp")[:my_rows]

    weighted = exact_dot(own, left_own, (1, 0))
    gram = jnp.dot(left_own.T, left_own, precision=HI)
    both = all_sum(jnp.concatenate([weighted, gram]), "tp")
    weighted, gram = both[: weighted.shape[0]], both[weighted.shape[0] :]
    left_own, weighted = lax.optimization_barrier((left_own, weighted))
    right_part = padded_rows(exact_dot(out_grads, weighted, (0, 0)), replicas)
    right_sum = gather_rows(scatter_sum(right_part, "dp"), "dp")[: out_grads.shape[1]]
    left_sum = gather_rows(left_own, "tp")

    gram = gram + 1e-06 * jnp.trace(gram) / rank * jnp.eye(rank, dtype=gram.dtype)
    lower = jnp.linalg.cholesky(gram)
    inverse = jax.scipy.linalg.solve_triangular(lower, jnp.eye(rank, dtype=gram.dtype), lower=True)
    left_basis = jnp.dot(left_sum, inverse.T, precision=HI)
    right_factor = jnp.dot(right_sum, inverse.T, precision=HI) / replicas

    left_top, left_low = bf16_terms(left_basis, 2)
    right_top, right_low = bf16_terms(right_factor, 2)
    tall = jnp.concatenate([activations.T, -left_top, -left_low, -left_top], 1)
    wide = jnp.concatenate([out_grads, right_top.T, right_top.T, right_low.T], 0)
    residual = jnp.dot(tall, wide, preferred_element_type=jnp.float32).astype(jnp.bfloat16)

    rows_dev = rows // replicas
    mine = lax.dynamic_slice_in_dim(left_basis, lax.axis_index("dp") * rows_dev, rows_dev, 0)
    update = jnp.dot(mine, right_factor.T, precision=HI)
    return (update, residual)


def solution(mesh):
    in_specs = (P("dp", None), P("dp", "tp"), P("tp", None))
    out_specs = (P("dp", "tp"), P("dp", "tp"))
    return jax.shard_map(
        per_device, mesh=mesh, in_specs=in_specs, out_specs=out_specs, check_vma=False
    )
```

```python
import functools

import jax
import jax.numpy as jnp
from jax import lax
from jax.experimental import pallas as pl
from jax.experimental.pallas import tpu as pltpu
from jax.sharding import PartitionSpec as P

HI = lax.Precision.HIGHEST


def factors_of(count):
    found, divisor = [], 2
    while count > 1:
        while count % divisor == 0:
            found.append(divisor)
            count //= divisor
        divisor += 1
    return found


def stages_of(axis):
    radices = []
    for factor in factors_of(lax.axis_size(axis)):
        if len(radices) > 1 and radices[-1] * factor <= 4:
            radices[-1] *= factor
        else:
            radices.append(factor)
    stages, stride = [], 1
    for radix in radices:
        stages.append((radix, stride))
        stride *= radix
    return stages


def partner(digit, step, radix):
    return digit ^ step if radix & (radix - 1) == 0 else (digit + step) % radix


def source(digit, step, radix):
    return digit ^ step if radix & (radix - 1) == 0 else (digit + radix - step) % radix


def shifted(value, axis, radix, stride, step):
    pairs = []
    for index in range(lax.axis_size(axis)):
        digit = index // stride % radix
        pairs.append((index, index + (partner(digit, step, radix) - digit) * stride))
    return lax.ppermute(value, axis, pairs)


def scatter_sum(value, axis):
    position = lax.axis_index(axis)
    for radix, stride in stages_of(axis):
        digit = position // stride % radix
        rows = value.shape[0] // radix
        received = []
        for step in range(1, radix):
            block = lax.dynamic_slice_in_dim(value, partner(digit, step, radix) * rows, rows, 0)
            received.append(shifted(block, axis, radix, stride, step))
        value = lax.dynamic_slice_in_dim(value, digit * rows, rows, 0)
        for block in received:
            value = value + block
    return value


def gather_rows(value, axis):
    position = lax.axis_index(axis)
    for radix, stride in reversed(stages_of(axis)):
        digit = position // stride % radix
        rows = value.shape[0]
        whole = jnp.zeros((radix * rows, value.shape[1]), value.dtype)
        received = [shifted(value, axis, radix, stride, step) for step in range(1, radix)]
        whole = lax.dynamic_update_slice_in_dim(whole, value, digit * rows, 0)
        for step, block in enumerate(received, 1):
            whole = lax.dynamic_update_slice_in_dim(whole, block, source(digit, step, radix) * rows, 0)
        value = whole
    return value


def padded_rows(value, multiple):
    extra = -value.shape[0] % multiple
    return jnp.pad(value, ((0, extra), (0, 0))) if extra else value


def inverse_factor_body(first, last, width, state_ref, out_ref):
    size = state_ref.shape[0]
    row = lax.broadcasted_iota(jnp.int32, (size, size), 0)
    column = lax.broadcasted_iota(jnp.int32, (size, size), 1)
    state = state_ref[...]
    if first == 0:
        diagonal = jnp.where(row == column, state, 0.0)
        ridge = 1e-06 * jnp.sum(diagonal) / size
        state = state + jnp.where(row == column, ridge, 0.0)
    out_ref[...] = state
    sub = lax.broadcasted_iota(jnp.int32, (width, size), 0)
    lane = lax.broadcasted_iota(jnp.int32, (width, size), 1)

    def spread(block, index):
        return jnp.broadcast_to(block[index : index + 1, :], (width, size))

    for start in range(first, last, width):
        stop = start + width
        block = out_ref[start:stop, :]
        columns = [
            jnp.broadcast_to(block[:, start + k : start + k + 1], (width, size)) for k in range(width)
        ]
        pivots = jnp.ones((width, size), jnp.float32)
        for j in range(width):
            pivot = spread(columns[j], j)
            pivots = jnp.where(sub == j, pivot, pivots)
            ratio = jnp.where(sub > j, columns[j] / pivot, 0.0)
            for k in range(width):
                if k != j:
                    columns[k] = columns[k] - ratio * spread(columns[k], j)
            columns[j] = jnp.where(sub == j, 1.0, -ratio)
        scale = 1.0 / jnp.sqrt(pivots)
        inside = (lane >= start) & (lane < stop)
        lead = jnp.where(inside, jnp.where(lane - start == sub, 1.0, 0.0), block)
        rows = columns[0] * spread(lead, 0)
        for k in range(1, width):
            rows = rows + columns[k] * spread(lead, k)
        rows = rows * scale
        out_ref[start:stop, :] = rows
        if stop < size:
            trail = jnp.where(lane >= stop, rows, 0.0)
            change = lax.dot_general(trail, rows, (((0,), (0,)), ((), ())), precision=HI, preferred_element_type=jnp.float32)
            rest = out_ref[stop:, :]
            hit = (column[stop:] >= start) & (column[stop:] < stop)
            out_ref[stop:, :] = jnp.where(hit, 0.0, rest) - change[stop:]
    if last == size:
        out_ref[...] = jnp.where(row >= column, out_ref[...], 0.0)


def inverse_factor(gram, pieces=2, width=16):
    size = gram.shape[0]
    state = gram
    for piece in range(pieces):
        first, last = size * piece // pieces, size * (piece + 1) // pieces
        call = pl.pallas_call(
            functools.partial(inverse_factor_body, first, last, width),
            out_shape=jax.ShapeDtypeStruct(gram.shape, jnp.float32),
            in_specs=[pl.BlockSpec(memory_space=pltpu.VMEM)],
            out_specs=pl.BlockSpec(memory_space=pltpu.VMEM),
            compiler_params=grant(4),
            cost_estimate=cost(3),
        )
        state = call(state)
    return state


def vmem(count):
    return [pl.BlockSpec(memory_space=pltpu.VMEM)] * count


SMEM = pl.BlockSpec(memory_space=pltpu.SMEM)


def grant(mebibytes, **more):
    return pltpu.CompilerParams(vmem_limit_bytes=mebibytes << 20, **more)


def cost(microseconds):
    return pl.CostEstimate(flops=int(microseconds * 1e9), bytes_accessed=1 << 17, transcendentals=0)


def terms_in_kernel(value, count):
    terms = []
    for _ in range(count):
        top = value.astype(jnp.bfloat16)
        terms.append(top)
        value = value - top.astype(jnp.float32)
    return terms


def exact_dot(narrow, wide, contract):
    dims = ((contract[:1], contract[1:]), ((), ()))
    total = None
    for term in reversed(terms_in_kernel(wide, 3)):
        part = lax.dot_general(narrow, term, dims, preferred_element_type=jnp.float32)
        total = part if total is None else total + part
    return total


def nt_dot(left, right):
    dims = (((1,), (1,)), ((), ()))
    return lax.dot_general(left, right, dims, precision=HI, preferred_element_type=jnp.float32)


def project_body(grads_ref, right_ref, out_ref):
    out_ref[...] = exact_dot(grads_ref[...], right_ref[...], (1, 0))


def project(out_grads, right_prev):
    return pl.pallas_call(
        project_body,
        out_shape=jax.ShapeDtypeStruct((out_grads.shape[0], right_prev.shape[1]), jnp.float32),
        in_specs=vmem(2),
        out_specs=vmem(1)[0],
        compiler_params=grant(12),
        name="project",
    )(out_grads, right_prev)


def apply_body(place_ref, tall_ref, *refs):
    total = refs[0][...]
    for ref in refs[1:-1]:
        total = total + ref[...]
    rows = refs[-1].shape[0]
    mine = pl.ds(pl.multiple_of(place_ref[0] * rows, rows), rows)
    refs[-1][...] = exact_dot(tall_ref[mine, :], total, (1, 0))


def apply(place, tall, rows, parts):
    return pl.pallas_call(
        apply_body,
        out_shape=jax.ShapeDtypeStruct((rows, parts[0].shape[1]), jnp.float32),
        in_specs=[SMEM] + vmem(1 + len(parts)),
        out_specs=vmem(1)[0],
        compiler_params=grant(12),
        name="apply",
    )(place, tall, *parts)


def weigh_body(place_ref, tall_ref, left_ref, out_ref):
    rows = left_ref.shape[0]
    mine = pl.ds(pl.multiple_of(place_ref[0] * rows, rows), rows)
    out_ref[...] = exact_dot(tall_ref[mine, :], left_ref[...], (0, 0))


def weigh(place, tall, left):
    return pl.pallas_call(
        weigh_body,
        out_shape=jax.ShapeDtypeStruct((tall.shape[1], left.shape[1]), jnp.float32),
        in_specs=[SMEM] + vmem(2),
        out_specs=vmem(1)[0],
        compiler_params=grant(12),
        name="weigh",
    )(place, tall, left)


def basis_body(place_ref, inverse_ref, acts_ref, *refs):
    out_ref, rank = refs[-1], inverse_ref.shape[0]
    tokens = acts_ref.shape[1]
    out_ref[:, :tokens] = acts_ref[...]
    for part, ref in enumerate(refs[:-1]):
        rows = ref.shape[0]
        top, low = terms_in_kernel(-nt_dot(ref[...], inverse_ref[...]), 2)
        where = pl.ds(pl.multiple_of(place_ref[part] * rows, rows), rows)
        for index, term in enumerate((top, low, top)):
            out_ref[where, tokens + index * rank : tokens + (index + 1) * rank] = term


def basis(places, inverse, acts, parts):
    columns = acts.shape[1] + 3 * inverse.shape[0]
    return pl.pallas_call(
        basis_body,
        out_shape=jax.ShapeDtypeStruct((acts.shape[0], columns), jnp.bfloat16),
        in_specs=[SMEM] + vmem(2 + len(parts)),
        out_specs=vmem(1)[0],
        compiler_params=grant(16),
        cost_estimate=cost(2),
        name="basis",
    )(places, inverse, acts, *parts)


def finish_body(replicas, mine_ref, tall_ref, grads_ref, sum_ref, inverse_ref, update_ref, residual_ref, wide):
    step, tile = pl.program_id(0), residual_ref.shape[0]
    tokens, rank = grads_ref.shape[0], inverse_ref.shape[0]

    @pl.when(step == 0)
    def _():
        right = nt_dot(inverse_ref[...], sum_ref[...]) * (1.0 / replicas)
        top, low = terms_in_kernel(right, 2)
        wide[:tokens, :] = grads_ref[...]
        for index, term in enumerate((top, top, low)):
            wide[tokens + index * rank : tokens + (index + 1) * rank, :] = term
        update_ref[...] = -jnp.dot(mine_ref[:, tokens:], wide[tokens:, :], preferred_element_type=jnp.float32)

    rows = pl.ds(pl.multiple_of(step * tile, tile), tile)
    residual = jnp.dot(tall_ref[rows, :], wide[...], preferred_element_type=jnp.float32)
    residual_ref[...] = residual.astype(jnp.bfloat16)


def finish(replicas, mine, tall, out_grads, right_sum, inverse):
    rows, columns = tall.shape[0], out_grads.shape[1]
    my_rows = mine.shape[0]
    tile = next(size for size in (384, 256, 192, 128, 96, 64, 32, 16, 8) if rows % size == 0)
    return pl.pallas_call(
        functools.partial(finish_body, replicas),
        grid=(rows // tile,),
        out_shape=(
            jax.ShapeDtypeStruct((my_rows, columns), jnp.float32),
            jax.ShapeDtypeStruct((rows, columns), jnp.bfloat16),
        ),
        in_specs=vmem(5),
        out_specs=(
            pl.BlockSpec((my_rows, columns), lambda i: (0, 0)),
            pl.BlockSpec((tile, columns), lambda i: (i, 0)),
        ),
        scratch_shapes=[pltpu.VMEM((tall.shape[1], columns), jnp.bfloat16)],
        compiler_params=grant(24, dimension_semantics=("arbitrary",)),
        name="finish",
    )(mine, tall, out_grads, right_sum, inverse)


def sent_all(value, axis):
    size, me = lax.axis_size(axis), lax.axis_index(axis)
    values, places = [value], [me]
    for step in range(1, size):
        values.append(shifted(value, axis, size, 1, step))
        places.append(source(me, step, size))
    return values, jnp.stack(places).astype(jnp.int32)


def per_device(activations, out_grads, right_prev):
    replicas, columns = lax.axis_size("dp"), lax.axis_size("tp")
    rows, my_columns = activations.shape[1], out_grads.shape[1]
    my_rows = rows // columns
    place = lax.axis_index("tp").astype(jnp.int32).reshape(1)
    origin = jnp.zeros((1,), jnp.int32)
    acts, grads = lax.optimization_barrier((activations.T, out_grads.T))

    projected, _ = sent_all(project(out_grads, right_prev), "tp")
    left_part = padded_rows(apply(place, acts, my_rows, projected), replicas)
    left_own = gather_rows(scatter_sum(left_part, "dp"), "dp")[:my_rows]

    weighted_own, left_own = lax.optimization_barrier((weigh(place, acts, left_own), left_own))
    weighted, _ = sent_all(weighted_own, "tp")
    gram = jnp.dot(left_own.T, left_own, precision=HI)
    grams, _ = sent_all(gram, "tp")
    gram = sum(grams[1:], grams[0])
    left_own, weighted[0] = lax.optimization_barrier((left_own, weighted[0]))
    right_part = padded_rows(apply(origin, grads, my_columns, weighted), replicas)
    right_sum = gather_rows(scatter_sum(right_part, "dp"), "dp")[:my_columns]

    parts, places = sent_all(left_own, "tp")
    inverse = inverse_factor(gram)
    tall = basis(places, inverse, acts, parts)
    rows_dev = rows // replicas
    mine = lax.dynamic_slice_in_dim(tall, lax.axis_index("dp") * rows_dev, rows_dev, 0)
    return finish(replicas, mine, tall, out_grads, right_sum, inverse)


def solution(mesh):
    in_specs = (P("dp", None), P("dp", "tp"), P("tp", None))
    out_specs = (P("dp", "tp"), P("dp", "tp"))
    return jax.shard_map(per_device, mesh=mesh, in_specs=in_specs, out_specs=out_specs, check_vma=False)
```

```python
import functools

import jax
import jax.numpy as jnp
from jax import lax
from jax.experimental import pallas as pl
from jax.experimental.pallas import tpu as pltpu
from jax.sharding import PartitionSpec as P

HI = lax.Precision.HIGHEST


def factors_of(count):
    found, divisor = [], 2
    while count > 1:
        while count % divisor == 0:
            found.append(divisor)
            count //= divisor
        divisor += 1
    return found


def stages_of(axis):
    radices = []
    for factor in factors_of(lax.axis_size(axis)):
        if len(radices) > 1 and radices[-1] * factor <= 4:
            radices[-1] *= factor
        else:
            radices.append(factor)
    stages, stride = [], 1
    for radix in radices:
        stages.append((radix, stride))
        stride *= radix
    return stages


def partner(digit, step, radix):
    return digit ^ step if radix & (radix - 1) == 0 else (digit + step) % radix


def source(digit, step, radix):
    return digit ^ step if radix & (radix - 1) == 0 else (digit + radix - step) % radix


def shifted(value, axis, radix, stride, step):
    pairs = []
    for index in range(lax.axis_size(axis)):
        digit = index // stride % radix
        pairs.append((index, index + (partner(digit, step, radix) - digit) * stride))
    return lax.ppermute(value, axis, pairs)


def scatter_sum(value, axis):
    position = lax.axis_index(axis)
    for radix, stride in stages_of(axis):
        digit = position // stride % radix
        rows = value.shape[0] // radix
        received = []
        for step in range(1, radix):
            block = lax.dynamic_slice_in_dim(value, partner(digit, step, radix) * rows, rows, 0)
            received.append(shifted(block, axis, radix, stride, step))
        value = lax.dynamic_slice_in_dim(value, digit * rows, rows, 0)
        for block in received:
            value = value + block
    return value


def gather_rows(value, axis):
    position = lax.axis_index(axis)
    for radix, stride in reversed(stages_of(axis)):
        digit = position // stride % radix
        rows = value.shape[0]
        whole = jnp.zeros((radix * rows, value.shape[1]), value.dtype)
        received = [shifted(value, axis, radix, stride, step) for step in range(1, radix)]
        whole = lax.dynamic_update_slice_in_dim(whole, value, digit * rows, 0)
        for step, block in enumerate(received, 1):
            whole = lax.dynamic_update_slice_in_dim(whole, block, source(digit, step, radix) * rows, 0)
        value = whole
    return value


def padded_rows(value, multiple):
    extra = -value.shape[0] % multiple
    return jnp.pad(value, ((0, extra), (0, 0))) if extra else value


def inverse_factor_body(first, last, width, state_ref, out_ref):
    size = state_ref.shape[0]
    row = lax.broadcasted_iota(jnp.int32, (size, size), 0)
    column = lax.broadcasted_iota(jnp.int32, (size, size), 1)
    state = state_ref[...]
    if first == 0:
        diagonal = jnp.where(row == column, state, 0.0)
        ridge = 1e-06 * jnp.sum(diagonal) / size
        state = state + jnp.where(row == column, ridge, 0.0)
    out_ref[...] = state
    sub = lax.broadcasted_iota(jnp.int32, (width, size), 0)
    lane = lax.broadcasted_iota(jnp.int32, (width, size), 1)

    def spread(block, index):
        return jnp.broadcast_to(block[index : index + 1, :], (width, size))

    for start in range(first, last, width):
        stop = start + width
        block = out_ref[start:stop, :]
        columns = [
            jnp.broadcast_to(block[:, start + k : start + k + 1], (width, size)) for k in range(width)
        ]
        pivots = jnp.ones((width, size), jnp.float32)
        for j in range(width):
            pivot = spread(columns[j], j)
            pivots = jnp.where(sub == j, pivot, pivots)
            ratio = jnp.where(sub > j, columns[j] / pivot, 0.0)
            for k in range(width):
                if k != j:
                    columns[k] = columns[k] - ratio * spread(columns[k], j)
            columns[j] = jnp.where(sub == j, 1.0, -ratio)
        scale = 1.0 / jnp.sqrt(pivots)
        inside = (lane >= start) & (lane < stop)
        lead = jnp.where(inside, jnp.where(lane - start == sub, 1.0, 0.0), block)
        rows = columns[0] * spread(lead, 0)
        for k in range(1, width):
            rows = rows + columns[k] * spread(lead, k)
        rows = rows * scale
        out_ref[start:stop, :] = rows
        if stop < size:
            trail = jnp.where(lane >= stop, rows, 0.0)
            change = lax.dot_general(trail, rows, (((0,), (0,)), ((), ())), precision=HI, preferred_element_type=jnp.float32)
            rest = out_ref[stop:, :]
            hit = (column[stop:] >= start) & (column[stop:] < stop)
            out_ref[stop:, :] = jnp.where(hit, 0.0, rest) - change[stop:]
    if last == size:
        out_ref[...] = jnp.where(row >= column, out_ref[...], 0.0)


def inverse_factor(gram, pieces=2, width=16):
    size = gram.shape[0]
    state = gram
    for piece in range(pieces):
        first, last = size * piece // pieces, size * (piece + 1) // pieces
        call = pl.pallas_call(
            functools.partial(inverse_factor_body, first, last, width),
            out_shape=jax.ShapeDtypeStruct(gram.shape, jnp.float32),
            in_specs=[pl.BlockSpec(memory_space=pltpu.VMEM)],
            out_specs=pl.BlockSpec(memory_space=pltpu.VMEM),
            compiler_params=grant(2),
            cost_estimate=cost(3),
        )
        state = call(state)
    return state


def vmem(count):
    return [pl.BlockSpec(memory_space=pltpu.VMEM)] * count


SMEM = pl.BlockSpec(memory_space=pltpu.SMEM)


def grant(mebibytes, **more):
    return pltpu.CompilerParams(vmem_limit_bytes=mebibytes << 20, **more)


def cost(microseconds):
    return pl.CostEstimate(flops=int(microseconds * 1e9), bytes_accessed=1 << 17, transcendentals=0)


def terms_in_kernel(value, count):
    terms = []
    for _ in range(count):
        top = value.astype(jnp.bfloat16)
        terms.append(top)
        value = value - top.astype(jnp.float32)
    return terms


def exact_dot(narrow, wide, contract):
    dims = ((contract[:1], contract[1:]), ((), ()))
    total = None
    for term in reversed(terms_in_kernel(wide, 3)):
        part = lax.dot_general(narrow, term, dims, preferred_element_type=jnp.float32)
        total = part if total is None else total + part
    return total


def nt_dot(left, right):
    dims = (((1,), (1,)), ((), ()))
    return lax.dot_general(left, right, dims, precision=HI, preferred_element_type=jnp.float32)


def project_body(grads_ref, right_ref, out_ref):
    out_ref[...] = exact_dot(grads_ref[...], right_ref[...], (1, 0))


def project(out_grads, right_prev):
    return pl.pallas_call(
        project_body,
        out_shape=jax.ShapeDtypeStruct((out_grads.shape[0], right_prev.shape[1]), jnp.float32),
        in_specs=vmem(2),
        out_specs=vmem(1)[0],
        compiler_params=grant(4),
        name="project",
    )(out_grads, right_prev)


def apply_body(place_ref, tall_ref, *refs):
    total = refs[0][...]
    for ref in refs[1:-1]:
        total = total + ref[...]
    rows = refs[-1].shape[0]
    mine = pl.ds(pl.multiple_of(place_ref[0] * rows, rows), rows)
    refs[-1][...] = exact_dot(tall_ref[mine, :], total, (1, 0))


def apply(place, tall, rows, parts):
    return pl.pallas_call(
        apply_body,
        out_shape=jax.ShapeDtypeStruct((rows, parts[0].shape[1]), jnp.float32),
        in_specs=[SMEM] + vmem(1 + len(parts)),
        out_specs=vmem(1)[0],
        compiler_params=grant(4),
        name="apply",
    )(place, tall, *parts)


def weigh_body(place_ref, tall_ref, left_ref, out_ref):
    rows = left_ref.shape[0]
    mine = pl.ds(pl.multiple_of(place_ref[0] * rows, rows), rows)
    out_ref[...] = exact_dot(tall_ref[mine, :], left_ref[...], (0, 0))


def weigh(place, tall, left):
    return pl.pallas_call(
        weigh_body,
        out_shape=jax.ShapeDtypeStruct((tall.shape[1], left.shape[1]), jnp.float32),
        in_specs=[SMEM] + vmem(2),
        out_specs=vmem(1)[0],
        compiler_params=grant(4),
        name="weigh",
    )(place, tall, left)


def basis_body(place_ref, inverse_ref, acts_ref, *refs):
    out_ref, rank = refs[-1], inverse_ref.shape[0]
    tokens = acts_ref.shape[1]
    out_ref[:, :tokens] = acts_ref[...]
    for part, ref in enumerate(refs[:-1]):
        rows = ref.shape[0]
        top, low = terms_in_kernel(-nt_dot(ref[...], inverse_ref[...]), 2)
        where = pl.ds(pl.multiple_of(place_ref[part] * rows, rows), rows)
        for index, term in enumerate((top, low, top)):
            out_ref[where, tokens + index * rank : tokens + (index + 1) * rank] = term


def basis(places, inverse, acts, parts):
    columns = acts.shape[1] + 3 * inverse.shape[0]
    return pl.pallas_call(
        basis_body,
        out_shape=jax.ShapeDtypeStruct((acts.shape[0], columns), jnp.bfloat16),
        in_specs=[SMEM] + vmem(2 + len(parts)),
        out_specs=vmem(1)[0],
        compiler_params=grant(8),
        cost_estimate=cost(2),
        name="basis",
    )(places, inverse, acts, *parts)


def finish_body(replicas, place_ref, mine_ref, tall_ref, grads_ref, sum_ref, inverse_ref, update_ref, residual_ref, wide):
    step, tile = pl.program_id(0), residual_ref.shape[0]
    tokens, rank = grads_ref.shape[0], inverse_ref.shape[0]

    @pl.when(step == 0)
    def _():
        right = nt_dot(inverse_ref[...], sum_ref[...]) * (1.0 / replicas)
        top, low = terms_in_kernel(right, 2)
        wide[:tokens, :] = grads_ref[...]
        for index, term in enumerate((top, top, low)):
            wide[tokens + index * rank : tokens + (index + 1) * rank, :] = term
        my_rows = update_ref.shape[0]
        mine = pl.ds(pl.multiple_of(place_ref[0] * my_rows, 16), my_rows)
        left = mine_ref[mine, tokens:] if my_rows % 16 == 0 else mine_ref[:, tokens:]
        update_ref[...] = -jnp.dot(left, wide[tokens:, :], preferred_element_type=jnp.float32)

    rows = pl.ds(pl.multiple_of(step * tile, tile), tile)
    residual = jnp.dot(tall_ref[rows, :], wide[...], preferred_element_type=jnp.float32)
    residual_ref[...] = residual.astype(jnp.bfloat16)


def finish(replicas, place, tall, out_grads, right_sum, inverse):
    rows, columns = tall.shape[0], out_grads.shape[1]
    my_rows, mine = rows // replicas, tall
    if my_rows % 16 != 0:
        mine = lax.dynamic_slice_in_dim(tall, place[0] * my_rows, my_rows, 0)
    tile = next(size for size in (384, 256, 192, 128, 96, 64, 32, 16, 8) if rows % size == 0)
    return pl.pallas_call(
        functools.partial(finish_body, replicas),
        grid=(rows // tile,),
        out_shape=(
            jax.ShapeDtypeStruct((my_rows, columns), jnp.float32),
            jax.ShapeDtypeStruct((rows, columns), jnp.bfloat16),
        ),
        in_specs=[SMEM] + vmem(5),
        out_specs=(
            pl.BlockSpec((my_rows, columns), lambda i: (0, 0)),
            pl.BlockSpec((tile, columns), lambda i: (i, 0)),
        ),
        scratch_shapes=[pltpu.VMEM((tall.shape[1], columns), jnp.bfloat16)],
        compiler_params=grant(12, dimension_semantics=("arbitrary",)),
        name="finish",
    )(place, mine, tall, out_grads, right_sum, inverse)


def sent_all(value, axis):
    size, me = lax.axis_size(axis), lax.axis_index(axis)
    values, places = [value], [me]
    for step in range(1, size):
        values.append(shifted(value, axis, size, 1, step))
        places.append(source(me, step, size))
    return values, jnp.stack(places).astype(jnp.int32)


def per_device(activations, out_grads, right_prev):
    replicas, columns = lax.axis_size("dp"), lax.axis_size("tp")
    rows, my_columns = activations.shape[1], out_grads.shape[1]
    my_rows = rows // columns
    place = lax.axis_index("tp").astype(jnp.int32).reshape(1)
    origin = jnp.zeros((1,), jnp.int32)
    acts, grads = lax.optimization_barrier((activations.T, out_grads.T))

    projected, _ = sent_all(project(out_grads, right_prev), "tp")
    left_part = padded_rows(apply(place, acts, my_rows, projected), replicas)
    left_own = gather_rows(scatter_sum(left_part, "dp"), "dp")[:my_rows]

    weighted_own, left_own = lax.optimization_barrier((weigh(place, acts, left_own), left_own))
    weighted, _ = sent_all(weighted_own, "tp")
    gram = jnp.dot(left_own.T, left_own, precision=HI)
    grams, _ = sent_all(gram, "tp")
    gram = sum(grams[1:], grams[0])
    left_own, weighted[0] = lax.optimization_barrier((left_own, weighted[0]))
    right_part = padded_rows(apply(origin, grads, my_columns, weighted), replicas)
    right_sum = gather_rows(scatter_sum(right_part, "dp"), "dp")[:my_columns]

    parts, places = sent_all(left_own, "tp")
    inverse = inverse_factor(gram)
    tall = basis(places, inverse, acts, parts)
    replica = lax.axis_index("dp").astype(jnp.int32).reshape(1)
    return finish(replicas, replica, tall, out_grads, right_sum, inverse)


def solution(mesh):
    in_specs = (P("dp", None), P("dp", "tp"), P("tp", None))
    out_specs = (P("dp", "tp"), P("dp", "tp"))
    return jax.shard_map(per_device, mesh=mesh, in_specs=in_specs, out_specs=out_specs, check_vma=False)
```

```python
import functools

import jax
import jax.numpy as jnp
from jax import lax
from jax.experimental import pallas as pl
from jax.experimental.pallas import tpu as pltpu
from jax.sharding import PartitionSpec as P

HI = lax.Precision.HIGHEST


def factors_of(count):
    found, divisor = [], 2
    while count > 1:
        while count % divisor == 0:
            found.append(divisor)
            count //= divisor
        divisor += 1
    return found


def stages_of(axis):
    radices = []
    for factor in factors_of(lax.axis_size(axis)):
        if len(radices) > 1 and radices[-1] * factor <= 4:
            radices[-1] *= factor
        else:
            radices.append(factor)
    stages, stride = [], 1
    for radix in radices:
        stages.append((radix, stride))
        stride *= radix
    return stages


def partner(digit, step, radix):
    return digit ^ step if radix & (radix - 1) == 0 else (digit + step) % radix


def source(digit, step, radix):
    return digit ^ step if radix & (radix - 1) == 0 else (digit + radix - step) % radix


def shifted(value, axis, radix, stride, step):
    pairs = []
    for index in range(lax.axis_size(axis)):
        digit = index // stride % radix
        pairs.append((index, index + (partner(digit, step, radix) - digit) * stride))
    return lax.ppermute(value, axis, pairs)


def scatter_sum(value, axis, tied=()):
    position, stages = lax.axis_index(axis), stages_of(axis)
    for stage, (radix, stride) in enumerate(stages[:-1]):
        digit = position // stride % radix
        rows = value.shape[0] // radix
        received = []
        for step in range(1, radix):
            block = lax.dynamic_slice_in_dim(value, partner(digit, step, radix) * rows, rows, 0)
            received.append(shifted(block, axis, radix, stride, step))
        value = lax.dynamic_slice_in_dim(value, digit * rows, rows, 0)
        for block in received:
            value = value + block
        if stage == 0:
            value, tied = lax.optimization_barrier((value, tied))
    radix, stride = stages[-1]
    received = [shifted(value, axis, radix, stride, step) for step in range(1, radix)]
    digit = position // stride % radix
    if radix == 2:
        return value + received[0], tied
    return ordered_sum([value] + received, digit), tied


def ordered_sum(values, digit):
    radix, total = len(values), None
    for place in range(radix):
        term = values[0]
        for step in range(1, radix):
            term = jnp.where(source(digit, step, radix) == place, values[step], term)
        total = term if total is None else total + term
    return total


def gather_rows(value, axis):
    position = lax.axis_index(axis)
    for radix, stride in reversed(stages_of(axis)[:-1]):
        digit = position // stride % radix
        rows = value.shape[0]
        whole = jnp.zeros((radix * rows, value.shape[1]), value.dtype)
        received = [shifted(value, axis, radix, stride, step) for step in range(1, radix)]
        whole = lax.dynamic_update_slice_in_dim(whole, value, digit * rows, 0)
        for step, block in enumerate(received, 1):
            whole = lax.dynamic_update_slice_in_dim(whole, block, source(digit, step, radix) * rows, 0)
        value = whole
    return value


def blocks_of(axis):
    return lax.axis_size(axis) // stages_of(axis)[-1][0]


def padded_rows(value, multiple):
    extra = -value.shape[0] % multiple
    return jnp.pad(value, ((0, extra), (0, 0))) if extra else value


def inverse_factor_body(first, last, width, state_ref, out_ref):
    size = state_ref.shape[0]
    row = lax.broadcasted_iota(jnp.int32, (size, size), 0)
    column = lax.broadcasted_iota(jnp.int32, (size, size), 1)
    state = state_ref[...]
    if first == 0:
        diagonal = jnp.where(row == column, state, 0.0)
        ridge = 1e-06 * jnp.sum(diagonal) / size
        state = state + jnp.where(row == column, ridge, 0.0)
    out_ref[...] = state
    sub = lax.broadcasted_iota(jnp.int32, (width, size), 0)
    lane = lax.broadcasted_iota(jnp.int32, (width, size), 1)

    def spread(block, index):
        return jnp.broadcast_to(block[index : index + 1, :], (width, size))

    for start in range(first, last, width):
        stop = start + width
        block = out_ref[start:stop, :]
        columns = [
            jnp.broadcast_to(block[:, start + k : start + k + 1], (width, size)) for k in range(width)
        ]
        pivots = jnp.ones((width, size), jnp.float32)
        for j in range(width):
            pivot = spread(columns[j], j)
            pivots = jnp.where(sub == j, pivot, pivots)
            ratio = jnp.where(sub > j, columns[j] / pivot, 0.0)
            for k in range(width):
                if k != j:
                    columns[k] = columns[k] - ratio * spread(columns[k], j)
            columns[j] = jnp.where(sub == j, 1.0, -ratio)
        scale = 1.0 / jnp.sqrt(pivots)
        inside = (lane >= start) & (lane < stop)
        lead = jnp.where(inside, jnp.where(lane - start == sub, 1.0, 0.0), block)
        rows = columns[0] * spread(lead, 0)
        for k in range(1, width):
            rows = rows + columns[k] * spread(lead, k)
        rows = rows * scale
        out_ref[start:stop, :] = rows
        if stop < size:
            trail = jnp.where(lane >= stop, rows, 0.0)
            change = lax.dot_general(trail, rows, (((0,), (0,)), ((), ())), precision=HI, preferred_element_type=jnp.float32)
            rest = out_ref[stop:, :]
            hit = (column[stop:] >= start) & (column[stop:] < stop)
            out_ref[stop:, :] = jnp.where(hit, 0.0, rest) - change[stop:]
    if last == size:
        out_ref[...] = jnp.where(row >= column, out_ref[...], 0.0)


def inverse_factor(gram, pieces=2, width=16):
    size = gram.shape[0]
    state = gram
    for piece in range(pieces):
        first, last = size * piece // pieces, size * (piece + 1) // pieces
        call = pl.pallas_call(
            functools.partial(inverse_factor_body, first, last, width),
            out_shape=jax.ShapeDtypeStruct(gram.shape, jnp.float32),
            in_specs=[pl.BlockSpec(memory_space=pltpu.VMEM)],
            out_specs=pl.BlockSpec(memory_space=pltpu.VMEM),
            compiler_params=grant(2),
            cost_estimate=cost(3),
        )
        state = call(state)
    return state


def vmem(count):
    return [pl.BlockSpec(memory_space=pltpu.VMEM)] * count


SMEM = pl.BlockSpec(memory_space=pltpu.SMEM)


def grant(mebibytes, **more):
    return pltpu.CompilerParams(vmem_limit_bytes=mebibytes << 20, **more)


def cost(microseconds):
    return pl.CostEstimate(flops=int(microseconds * 1e9), bytes_accessed=1 << 17, transcendentals=0)


def terms_in_kernel(value, count):
    terms = []
    for _ in range(count):
        top = value.astype(jnp.bfloat16)
        terms.append(top)
        value = value - top.astype(jnp.float32)
    return terms


def exact_dot(narrow, wide, contract):
    dims = ((contract[:1], contract[1:]), ((), ()))
    total = None
    for term in reversed(terms_in_kernel(wide, 3)):
        part = lax.dot_general(narrow, term, dims, preferred_element_type=jnp.float32)
        total = part if total is None else total + part
    return total


def nt_dot(left, right):
    dims = (((1,), (1,)), ((), ()))
    return lax.dot_general(left, right, dims, precision=HI, preferred_element_type=jnp.float32)


def project_body(grads_ref, right_ref, out_ref):
    out_ref[...] = exact_dot(grads_ref[...], right_ref[...], (1, 0))


def project(out_grads, right_prev):
    return pl.pallas_call(
        project_body,
        out_shape=jax.ShapeDtypeStruct((out_grads.shape[0], right_prev.shape[1]), jnp.float32),
        in_specs=vmem(2),
        out_specs=vmem(1)[0],
        compiler_params=grant(4),
        name="project",
    )(out_grads, right_prev)


def apply_body(place_ref, tall_ref, *refs):
    total = refs[0][...]
    for ref in refs[1:-1]:
        total = total + ref[...]
    rows = refs[-1].shape[0]
    mine = pl.ds(pl.multiple_of(place_ref[0] * rows, rows), rows)
    refs[-1][...] = exact_dot(tall_ref[mine, :], total, (1, 0))


def apply(place, tall, rows, parts):
    return pl.pallas_call(
        apply_body,
        out_shape=jax.ShapeDtypeStruct((rows, parts[0].shape[1]), jnp.float32),
        in_specs=[SMEM] + vmem(1 + len(parts)),
        out_specs=vmem(1)[0],
        compiler_params=grant(4),
        name="apply",
    )(place, tall, *parts)


def weigh_body(place_ref, tall_ref, left_ref, out_ref):
    rows = left_ref.shape[0]
    mine = pl.ds(pl.multiple_of(place_ref[0] * rows, rows), rows)
    out_ref[...] = exact_dot(tall_ref[mine, :], left_ref[...], (0, 0))


def weigh(place, tall, left):
    return pl.pallas_call(
        weigh_body,
        out_shape=jax.ShapeDtypeStruct((tall.shape[1], left.shape[1]), jnp.float32),
        in_specs=[SMEM] + vmem(2),
        out_specs=vmem(1)[0],
        compiler_params=grant(4),
        name="weigh",
    )(place, tall, left)


def basis_body(place_ref, inverse_ref, acts_ref, *refs):
    out_ref, rank = refs[-1], inverse_ref.shape[0]
    tokens = acts_ref.shape[1]
    out_ref[:, :tokens] = acts_ref[...]
    for part, ref in enumerate(refs[:-1]):
        rows = ref.shape[0]
        top, low = terms_in_kernel(-nt_dot(ref[...], inverse_ref[...]), 2)
        where = pl.ds(pl.multiple_of(place_ref[part] * rows, rows), rows)
        for index, term in enumerate((top, low, top)):
            out_ref[where, tokens + index * rank : tokens + (index + 1) * rank] = term


def basis(places, inverse, acts, parts):
    columns = acts.shape[1] + 3 * inverse.shape[0]
    return pl.pallas_call(
        basis_body,
        out_shape=jax.ShapeDtypeStruct((acts.shape[0], columns), jnp.bfloat16),
        in_specs=[SMEM] + vmem(2 + len(parts)),
        out_specs=vmem(1)[0],
        compiler_params=grant(8),
        cost_estimate=cost(2),
        name="basis",
    )(places, inverse, acts, *parts)


def finish_body(replicas, place_ref, mine_ref, tall_ref, grads_ref, sum_ref, inverse_ref, update_ref, residual_ref, wide):
    step, tile = pl.program_id(0), residual_ref.shape[0]
    tokens, rank = grads_ref.shape[0], inverse_ref.shape[0]

    @pl.when(step == 0)
    def _():
        right = nt_dot(inverse_ref[...], sum_ref[...]) * (1.0 / replicas)
        top, low = terms_in_kernel(right, 2)
        wide[:tokens, :] = grads_ref[...]
        for index, term in enumerate((top, top, low)):
            wide[tokens + index * rank : tokens + (index + 1) * rank, :] = term
        my_rows = update_ref.shape[0]
        mine = pl.ds(pl.multiple_of(place_ref[0] * my_rows, 16), my_rows)
        left = mine_ref[mine, tokens:] if my_rows % 16 == 0 else mine_ref[:, tokens:]
        update_ref[...] = -jnp.dot(left, wide[tokens:, :], preferred_element_type=jnp.float32)

    rows = pl.ds(pl.multiple_of(step * tile, tile), tile)
    residual = jnp.dot(tall_ref[rows, :], wide[...], preferred_element_type=jnp.float32)
    residual_ref[...] = residual.astype(jnp.bfloat16)


def finish(replicas, place, tall, out_grads, right_sum, inverse):
    rows, columns = tall.shape[0], out_grads.shape[1]
    my_rows, mine = rows // replicas, tall
    if my_rows % 16 != 0:
        mine = lax.dynamic_slice_in_dim(tall, place[0] * my_rows, my_rows, 0)
    tile = next(size for size in (384, 256, 192, 128, 96, 64, 32, 16, 8) if rows % size == 0)
    return pl.pallas_call(
        functools.partial(finish_body, replicas),
        grid=(rows // tile,),
        out_shape=(
            jax.ShapeDtypeStruct((my_rows, columns), jnp.float32),
            jax.ShapeDtypeStruct((rows, columns), jnp.bfloat16),
        ),
        in_specs=[SMEM] + vmem(5),
        out_specs=(
            pl.BlockSpec((my_rows, columns), lambda i: (0, 0)),
            pl.BlockSpec((tile, columns), lambda i: (i, 0)),
        ),
        scratch_shapes=[pltpu.VMEM((tall.shape[1], columns), jnp.bfloat16)],
        compiler_params=grant(12, dimension_semantics=("arbitrary",)),
        name="finish",
    )(place, mine, tall, out_grads, right_sum, inverse)


def sent_all(value, axis):
    size, me = lax.axis_size(axis), lax.axis_index(axis)
    values, places = [value], [me]
    for step in range(1, size):
        values.append(shifted(value, axis, size, 1, step))
        places.append(source(me, step, size))
    return values, jnp.stack(places).astype(jnp.int32)


def per_device(activations, out_grads, right_prev):
    replicas, columns = lax.axis_size("dp"), lax.axis_size("tp")
    rows, my_columns = activations.shape[1], out_grads.shape[1]
    my_rows = rows // columns
    place = lax.axis_index("tp").astype(jnp.int32).reshape(1)
    origin = jnp.zeros((1,), jnp.int32)
    acts, grads = lax.optimization_barrier((activations.T, out_grads.T))

    projected, _ = sent_all(project(out_grads, right_prev), "tp")
    left_part = padded_rows(apply(place, acts, my_rows, projected), blocks_of("dp"))
    left_own, _ = scatter_sum(left_part, "dp")
    left_own = gather_rows(left_own, "dp")[:my_rows]

    weighted_own, left_own = lax.optimization_barrier((weigh(place, acts, left_own), left_own))
    weighted, _ = sent_all(weighted_own, "tp")
    gram = jnp.dot(left_own.T, left_own, precision=HI)
    grams, _ = sent_all(gram, "tp")
    left_own, weighted[0] = lax.optimization_barrier((left_own, weighted[0]))
    right_part = apply(origin, grads, my_columns, weighted)
    right_part = padded_rows(right_part, blocks_of("dp"))
    right_sum, grams = scatter_sum(right_part, "dp", tied=grams)
    right_sum = gather_rows(right_sum, "dp")[:my_columns]
    gram = sum(grams[1:], grams[0])

    parts, places = sent_all(left_own, "tp")
    inverse = inverse_factor(gram)
    tall = basis(places, inverse, acts, parts)
    replica = lax.axis_index("dp").astype(jnp.int32).reshape(1)
    return finish(replicas, replica, tall, out_grads, right_sum, inverse)


def solution(mesh):
    in_specs = (P("dp", None), P("dp", "tp"), P("tp", None))
    out_specs = (P("dp", "tp"), P("dp", "tp"))
    return jax.shard_map(per_device, mesh=mesh, in_specs=in_specs, out_specs=out_specs, check_vma=False)
```

```python
import functools

import jax
import jax.numpy as jnp
from jax import lax
from jax.experimental import pallas as pl
from jax.experimental.pallas import tpu as pltpu
from jax.sharding import PartitionSpec as P

HI = lax.Precision.HIGHEST


def factors_of(count):
    found, divisor = [], 2
    while count > 1:
        while count % divisor == 0:
            found.append(divisor)
            count //= divisor
        divisor += 1
    return found


def stages_of(axis):
    radices = []
    for factor in factors_of(lax.axis_size(axis)):
        if len(radices) > 1 and radices[-1] * factor <= 4:
            radices[-1] *= factor
        else:
            radices.append(factor)
    stages, stride = [], 1
    for radix in radices:
        stages.append((radix, stride))
        stride *= radix
    return stages


def partner(digit, step, radix):
    return digit ^ step if radix & (radix - 1) == 0 else (digit + step) % radix


def source(digit, step, radix):
    return digit ^ step if radix & (radix - 1) == 0 else (digit + radix - step) % radix


def shifted(value, axis, radix, stride, step):
    pairs = []
    for index in range(lax.axis_size(axis)):
        digit = index // stride % radix
        pairs.append((index, index + (partner(digit, step, radix) - digit) * stride))
    return lax.ppermute(value, axis, pairs)


def scatter_sum(value, axis, tied=()):
    position, stages = lax.axis_index(axis), stages_of(axis)
    for stage, (radix, stride) in enumerate(stages[:-1]):
        digit = position // stride % radix
        rows = value.shape[0] // radix
        received = []
        for step in range(1, radix):
            block = lax.dynamic_slice_in_dim(value, partner(digit, step, radix) * rows, rows, 0)
            received.append(shifted(block, axis, radix, stride, step))
        value = lax.dynamic_slice_in_dim(value, digit * rows, rows, 0)
        for block in received:
            value = value + block
        if stage == 0:
            value, tied = lax.optimization_barrier((value, tied))
    radix, stride = stages[-1]
    received = [shifted(value, axis, radix, stride, step) for step in range(1, radix)]
    return [value] + received, tied


def together(values, axis):
    radix, stride = stages_of(axis)[-1]
    if radix == 2:
        return values[0] + values[1]
    return ordered_sum(values, lax.axis_index(axis) // stride % radix)


def ordered_sum(values, digit):
    radix, total = len(values), None
    for place in range(radix):
        term = values[0]
        for step in range(1, radix):
            term = jnp.where(source(digit, step, radix) == place, values[step], term)
        total = term if total is None else total + term
    return total


def gather_rows(value, axis):
    position = lax.axis_index(axis)
    for radix, stride in reversed(stages_of(axis)[:-1]):
        digit = position // stride % radix
        rows = value.shape[0]
        whole = jnp.zeros((radix * rows, value.shape[1]), value.dtype)
        received = [shifted(value, axis, radix, stride, step) for step in range(1, radix)]
        whole = lax.dynamic_update_slice_in_dim(whole, value, digit * rows, 0)
        for step, block in enumerate(received, 1):
            whole = lax.dynamic_update_slice_in_dim(whole, block, source(digit, step, radix) * rows, 0)
        value = whole
    return value


def blocks_of(axis):
    return lax.axis_size(axis) // stages_of(axis)[-1][0]


def padded_rows(value, multiple):
    extra = -value.shape[0] % multiple
    return jnp.pad(value, ((0, extra), (0, 0))) if extra else value


def inverse_factor_body(first, last, width, state_ref, out_ref):
    size = state_ref.shape[0]
    row = lax.broadcasted_iota(jnp.int32, (size, size), 0)
    column = lax.broadcasted_iota(jnp.int32, (size, size), 1)
    state = state_ref[...]
    if first == 0:
        diagonal = jnp.where(row == column, state, 0.0)
        ridge = 1e-06 * jnp.sum(diagonal) / size
        state = state + jnp.where(row == column, ridge, 0.0)
    out_ref[...] = state
    sub = lax.broadcasted_iota(jnp.int32, (width, size), 0)
    lane = lax.broadcasted_iota(jnp.int32, (width, size), 1)

    def spread(block, index):
        return jnp.broadcast_to(block[index : index + 1, :], (width, size))

    for start in range(first, last, width):
        stop = start + width
        block = out_ref[start:stop, :]
        columns = [
            jnp.broadcast_to(block[:, start + k : start + k + 1], (width, size)) for k in range(width)
        ]
        pivots = jnp.ones((width, size), jnp.float32)
        for j in range(width):
            pivot = spread(columns[j], j)
            pivots = jnp.where(sub == j, pivot, pivots)
            ratio = jnp.where(sub > j, columns[j] / pivot, 0.0)
            for k in range(width):
                if k != j:
                    columns[k] = columns[k] - ratio * spread(columns[k], j)
            columns[j] = jnp.where(sub == j, 1.0, -ratio)
        scale = 1.0 / jnp.sqrt(pivots)
        inside = (lane >= start) & (lane < stop)
        lead = jnp.where(inside, jnp.where(lane - start == sub, 1.0, 0.0), block)
        rows = columns[0] * spread(lead, 0)
        for k in range(1, width):
            rows = rows + columns[k] * spread(lead, k)
        rows = rows * scale
        out_ref[start:stop, :] = rows
        if stop < size:
            trail = jnp.where(lane >= stop, rows, 0.0)
            change = lax.dot_general(trail, rows, (((0,), (0,)), ((), ())), precision=HI, preferred_element_type=jnp.float32)
            rest = out_ref[stop:, :]
            hit = (column[stop:] >= start) & (column[stop:] < stop)
            out_ref[stop:, :] = jnp.where(hit, 0.0, rest) - change[stop:]
    if last == size:
        out_ref[...] = jnp.where(row >= column, out_ref[...], 0.0)


def inverse_factor(gram, pieces=2, width=16):
    size = gram.shape[0]
    state = gram
    for piece in range(pieces):
        first, last = size * piece // pieces, size * (piece + 1) // pieces
        call = pl.pallas_call(
            functools.partial(inverse_factor_body, first, last, width),
            out_shape=jax.ShapeDtypeStruct(gram.shape, jnp.float32),
            in_specs=[pl.BlockSpec(memory_space=pltpu.VMEM)],
            out_specs=pl.BlockSpec(memory_space=pltpu.VMEM),
            compiler_params=grant(2),
            cost_estimate=cost(3),
        )
        state = call(state)
    return state


def vmem(count):
    return [pl.BlockSpec(memory_space=pltpu.VMEM)] * count


SMEM = pl.BlockSpec(memory_space=pltpu.SMEM)


def grant(mebibytes, **more):
    return pltpu.CompilerParams(vmem_limit_bytes=mebibytes << 20, **more)


def cost(microseconds):
    return pl.CostEstimate(flops=int(microseconds * 1e9), bytes_accessed=1 << 17, transcendentals=0)


def terms_in_kernel(value, count):
    terms = []
    for _ in range(count):
        top = value.astype(jnp.bfloat16)
        terms.append(top)
        value = value - top.astype(jnp.float32)
    return terms


def exact_dot(narrow, wide, contract):
    dims = ((contract[:1], contract[1:]), ((), ()))
    total = None
    for term in reversed(terms_in_kernel(wide, 3)):
        part = lax.dot_general(narrow, term, dims, preferred_element_type=jnp.float32)
        total = part if total is None else total + part
    return total


def nt_dot(left, right):
    dims = (((1,), (1,)), ((), ()))
    return lax.dot_general(left, right, dims, precision=HI, preferred_element_type=jnp.float32)


def project_body(grads_ref, right_ref, out_ref, grads, right, arrived):
    copies = [
        pltpu.make_async_copy(grads_ref, grads, arrived.at[0]),
        pltpu.make_async_copy(right_ref, right, arrived.at[1]),
    ]
    for copy in copies:
        copy.start()
    for copy in copies:
        copy.wait()
    out_ref[...] = exact_dot(grads[...], right[...], (1, 0))


def project(out_grads, right_prev):
    return pl.pallas_call(
        project_body,
        out_shape=jax.ShapeDtypeStruct((out_grads.shape[0], right_prev.shape[1]), jnp.float32),
        in_specs=[pl.BlockSpec(memory_space=pltpu.HBM)] * 2,
        out_specs=vmem(1)[0],
        scratch_shapes=[
            pltpu.VMEM(out_grads.shape, out_grads.dtype),
            pltpu.VMEM(right_prev.shape, right_prev.dtype),
            pltpu.SemaphoreType.DMA((2,)),
        ],
        compiler_params=grant(6),
        name="project",
    )(*(pltpu.with_memory_space_constraint(array, pltpu.HBM) for array in (out_grads, right_prev)))


def apply_body(place_ref, tall_ref, *refs):
    total = refs[0][...]
    for ref in refs[1:-1]:
        total = total + ref[...]
    rows = refs[-1].shape[0]
    mine = pl.ds(pl.multiple_of(place_ref[0] * rows, rows), rows)
    refs[-1][...] = exact_dot(tall_ref[mine, :], total, (1, 0))


def apply(place, tall, rows, parts):
    return pl.pallas_call(
        apply_body,
        out_shape=jax.ShapeDtypeStruct((rows, parts[0].shape[1]), jnp.float32),
        in_specs=[SMEM] + vmem(1 + len(parts)),
        out_specs=vmem(1)[0],
        compiler_params=grant(4),
        name="apply",
    )(place, tall, *parts)


def weigh_body(place_ref, tall_ref, left_ref, out_ref):
    rows = left_ref.shape[0]
    mine = pl.ds(pl.multiple_of(place_ref[0] * rows, rows), rows)
    out_ref[...] = exact_dot(tall_ref[mine, :], left_ref[...], (0, 0))


def weigh(place, tall, left):
    return pl.pallas_call(
        weigh_body,
        out_shape=jax.ShapeDtypeStruct((tall.shape[1], left.shape[1]), jnp.float32),
        in_specs=[SMEM] + vmem(2),
        out_specs=vmem(1)[0],
        compiler_params=grant(4),
        name="weigh",
    )(place, tall, left)


def basis_body(place_ref, inverse_ref, acts_ref, *refs):
    out_ref, rank = refs[-1], inverse_ref.shape[0]
    tokens = acts_ref.shape[1]
    out_ref[:, :tokens] = acts_ref[...]
    for part, ref in enumerate(refs[:-1]):
        rows = ref.shape[0]
        top, low = terms_in_kernel(-nt_dot(ref[...], inverse_ref[...]), 2)
        where = pl.ds(pl.multiple_of(place_ref[part] * rows, rows), rows)
        for index, term in enumerate((top, low, top)):
            out_ref[where, tokens + index * rank : tokens + (index + 1) * rank] = term


def basis(places, inverse, acts, parts):
    columns = acts.shape[1] + 3 * inverse.shape[0]
    return pl.pallas_call(
        basis_body,
        out_shape=jax.ShapeDtypeStruct((acts.shape[0], columns), jnp.bfloat16),
        in_specs=[SMEM] + vmem(2 + len(parts)),
        out_specs=vmem(1)[0],
        compiler_params=grant(8),
        cost_estimate=cost(2),
        name="basis",
    )(places, inverse, acts, *parts)


def blocks_fit(columns, axis):
    blocks = blocks_of(axis)
    return columns % blocks == 0 and columns // blocks % 128 == 0


def turn_body(replicas, inverse_ref, *refs):
    total = refs[0][...]
    for ref in refs[1:-1]:
        total = total + ref[...]
    right = nt_dot(total, inverse_ref[...]) * (1.0 / replicas)
    refs[-1][...] = jnp.transpose(right)


def turn(replicas, inverse, parts):
    rows, rank = parts[0].shape
    return pl.pallas_call(
        functools.partial(turn_body, replicas),
        out_shape=jax.ShapeDtypeStruct((rank, rows), jnp.float32),
        in_specs=vmem(1 + len(parts)),
        out_specs=vmem(1)[0],
        compiler_params=grant(2),
        name="turn",
    )(inverse, *parts)


def finish_body(replicas, turned, place_ref, mine_ref, tall_ref, grads_ref, sum_ref, inverse_ref, update_ref, residual_ref,
                wide, tiles, update, sent):
    tokens, rank = grads_ref.shape[0], inverse_ref.shape[0]
    count, tile = tiles.shape[:2]
    wide[:tokens, :] = grads_ref[...]
    width = sum_ref.shape[1] if turned else wide.shape[1]
    for start in range(0, wide.shape[1], width):
        if turned:
            first = start // width * rank
            top, low = terms_in_kernel(sum_ref[first : first + rank, :], 2)
        else:
            right = nt_dot(sum_ref[...], inverse_ref[...]) * (1.0 / replicas)
            top, low = (jnp.transpose(term) for term in terms_in_kernel(right, 2))
        for index, term in enumerate((top, top, low)):
            wide[tokens + index * rank : tokens + (index + 1) * rank, start : start + width] = term
    copies = []
    for index in range(count):
        rows = pl.ds(index * tile, tile)
        residual = jnp.dot(tall_ref[rows, :], wide[...], preferred_element_type=jnp.float32)
        tiles[index] = residual.astype(jnp.bfloat16)
        copies.append(pltpu.make_async_copy(tiles.at[index], residual_ref.at[rows, :], sent.at[index]))
        copies[-1].start()
        if index == 0:
            my_rows = update_ref.shape[0]
            mine = pl.ds(pl.multiple_of(place_ref[0] * my_rows, 16), my_rows)
            left = mine_ref[mine, tokens:] if my_rows % 16 == 0 else mine_ref[:, tokens:]
            update[...] = -jnp.dot(left, wide[tokens:, :], preferred_element_type=jnp.float32)
            copies.append(pltpu.make_async_copy(update, update_ref, sent.at[count]))
            copies[-1].start()
    for copy in copies:
        copy.wait()


def finish(replicas, turned, place, tall, out_grads, right_sum, inverse):
    rows, columns = tall.shape[0], out_grads.shape[1]
    my_rows, mine = rows // replicas, tall
    if my_rows % 16 != 0:
        mine = lax.dynamic_slice_in_dim(tall, place[0] * my_rows, my_rows, 0)
    tile = next(size for size in (256, 192, 128, 96, 64, 32, 16) if rows % size == 0)
    hbm = pl.BlockSpec(memory_space=pltpu.HBM)
    return pl.pallas_call(
        functools.partial(finish_body, replicas, turned),
        out_shape=(
            jax.ShapeDtypeStruct((my_rows, columns), jnp.float32),
            jax.ShapeDtypeStruct((rows, columns), jnp.bfloat16),
        ),
        in_specs=[SMEM] + vmem(5),
        out_specs=(hbm, hbm),
        scratch_shapes=[
            pltpu.VMEM((tall.shape[1], columns), jnp.bfloat16),
            pltpu.VMEM((rows // tile, tile, columns), jnp.bfloat16),
            pltpu.VMEM((my_rows, columns), jnp.float32),
            pltpu.SemaphoreType.DMA((rows // tile + 1,)),
        ],
        compiler_params=grant(20),
        name="finish",
    )(place, mine, tall, out_grads, right_sum, inverse)


def sent_all(value, axis):
    size, me = lax.axis_size(axis), lax.axis_index(axis)
    values, places = [value], [me]
    for step in range(1, size):
        values.append(shifted(value, axis, size, 1, step))
        places.append(source(me, step, size))
    return values, jnp.stack(places).astype(jnp.int32)


def per_device(activations, out_grads, right_prev):
    replicas, columns = lax.axis_size("dp"), lax.axis_size("tp")
    rows, my_columns = activations.shape[1], out_grads.shape[1]
    my_rows = rows // columns
    place = lax.axis_index("tp").astype(jnp.int32).reshape(1)
    origin = jnp.zeros((1,), jnp.int32)
    acts, grads = lax.optimization_barrier((activations.T, out_grads.T))

    projected, _ = sent_all(project(out_grads, right_prev), "tp")
    left_part = padded_rows(apply(place, acts, my_rows, projected), blocks_of("dp"))
    left_parts, _ = scatter_sum(left_part, "dp")
    left_own = gather_rows(together(left_parts, "dp"), "dp")[:my_rows]

    weighted_own, left_own = lax.optimization_barrier((weigh(place, acts, left_own), left_own))
    weighted, _ = sent_all(weighted_own, "tp")
    gram = jnp.dot(left_own.T, left_own, precision=HI)
    grams, _ = sent_all(gram, "tp")
    left_own, weighted[0] = lax.optimization_barrier((left_own, weighted[0]))
    right_part = apply(origin, grads, my_columns, weighted)
    right_part = padded_rows(right_part, blocks_of("dp"))
    right_parts, grams = scatter_sum(right_part, "dp", tied=grams)
    gram = sum(grams[1:], grams[0])

    parts, places = sent_all(left_own, "tp")
    inverse = inverse_factor(gram)
    turned = blocks_fit(my_columns, "dp") and len(right_parts) == 2
    right_own = turn(replicas, inverse, right_parts) if turned else together(right_parts, "dp")
    right_sum = gather_rows(right_own, "dp")
    right_sum = right_sum if turned else right_sum[:my_columns]
    tall = basis(places, inverse, acts, parts)
    replica = lax.axis_index("dp").astype(jnp.int32).reshape(1)
    return finish(replicas, turned, replica, tall, out_grads, right_sum, inverse)


def solution(mesh):
    in_specs = (P("dp", None), P("dp", "tp"), P("tp", None))
    out_specs = (P("dp", "tp"), P("dp", "tp"))
    return jax.shard_map(per_device, mesh=mesh, in_specs=in_specs, out_specs=out_specs, check_vma=False)
```

```python
import functools

import jax
import jax.numpy as jnp
from jax import lax
from jax.experimental import pallas as pl
from jax.experimental.pallas import tpu as pltpu
from jax.sharding import PartitionSpec as P

HI = lax.Precision.HIGHEST


def factors_of(count):
    found, divisor = [], 2
    while count > 1:
        while count % divisor == 0:
            found.append(divisor)
            count //= divisor
        divisor += 1
    return found


def stages_of(axis):
    radices = []
    for factor in factors_of(lax.axis_size(axis)):
        if len(radices) > 1 and radices[-1] * factor <= 4:
            radices[-1] *= factor
        else:
            radices.append(factor)
    stages, stride = [], 1
    for radix in radices:
        stages.append((radix, stride))
        stride *= radix
    return stages


def partner(digit, step, radix):
    return digit ^ step if radix & (radix - 1) == 0 else (digit + step) % radix


def source(digit, step, radix):
    return digit ^ step if radix & (radix - 1) == 0 else (digit + radix - step) % radix


def shifted(value, axis, radix, stride, step):
    pairs = []
    for index in range(lax.axis_size(axis)):
        digit = index // stride % radix
        pairs.append((index, index + (partner(digit, step, radix) - digit) * stride))
    return lax.ppermute(value, axis, pairs)


def scatter_sum(value, axis, tied=()):
    position, stages = lax.axis_index(axis), stages_of(axis)
    for stage, (radix, stride) in enumerate(stages[:-1]):
        digit = position // stride % radix
        rows = value.shape[0] // radix
        received = []
        for step in range(1, radix):
            block = lax.dynamic_slice_in_dim(value, partner(digit, step, radix) * rows, rows, 0)
            received.append(shifted(block, axis, radix, stride, step))
        value = lax.dynamic_slice_in_dim(value, digit * rows, rows, 0)
        for block in received:
            value = value + block
        if stage == 0:
            value, tied = lax.optimization_barrier((value, tied))
    radix, stride = stages[-1]
    received = [shifted(value, axis, radix, stride, step) for step in range(1, radix)]
    return [value] + received, tied


def together(values, axis):
    radix, stride = stages_of(axis)[-1]
    if radix == 2:
        return values[0] + values[1]
    return ordered_sum(values, lax.axis_index(axis) // stride % radix)


def ordered_sum(values, digit):
    radix, total = len(values), None
    for place in range(radix):
        term = values[0]
        for step in range(1, radix):
            term = jnp.where(source(digit, step, radix) == place, values[step], term)
        total = term if total is None else total + term
    return total


def gather_rows(value, axis):
    position = lax.axis_index(axis)
    for radix, stride in reversed(stages_of(axis)[:-1]):
        digit = position // stride % radix
        rows = value.shape[0]
        whole = jnp.zeros((radix * rows, value.shape[1]), value.dtype)
        received = [shifted(value, axis, radix, stride, step) for step in range(1, radix)]
        whole = lax.dynamic_update_slice_in_dim(whole, value, digit * rows, 0)
        for step, block in enumerate(received, 1):
            whole = lax.dynamic_update_slice_in_dim(whole, block, source(digit, step, radix) * rows, 0)
        value = whole
    return value


def blocks_of(axis):
    return lax.axis_size(axis) // stages_of(axis)[-1][0]


def padded_rows(value, multiple):
    extra = -value.shape[0] % multiple
    return jnp.pad(value, ((0, extra), (0, 0))) if extra else value


def inverse_factor_body(first, last, width, state_ref, out_ref):
    size = state_ref.shape[0]
    row = lax.broadcasted_iota(jnp.int32, (size, size), 0)
    column = lax.broadcasted_iota(jnp.int32, (size, size), 1)
    state = state_ref[...]
    if first == 0:
        diagonal = jnp.where(row == column, state, 0.0)
        ridge = 1e-06 * jnp.sum(diagonal) / size
        state = state + jnp.where(row == column, ridge, 0.0)
    out_ref[...] = state
    sub = lax.broadcasted_iota(jnp.int32, (width, size), 0)
    lane = lax.broadcasted_iota(jnp.int32, (width, size), 1)

    def spread(block, index):
        return jnp.broadcast_to(block[index : index + 1, :], (width, size))

    for start in range(first, last, width):
        stop = start + width
        block = out_ref[start:stop, :]
        columns = [
            jnp.broadcast_to(block[:, start + k : start + k + 1], (width, size)) for k in range(width)
        ]
        pivots = jnp.ones((width, size), jnp.float32)
        for j in range(width):
            pivot = spread(columns[j], j)
            pivots = jnp.where(sub == j, pivot, pivots)
            ratio = jnp.where(sub > j, columns[j] / pivot, 0.0)
            for k in range(width):
                if k != j:
                    columns[k] = columns[k] - ratio * spread(columns[k], j)
            columns[j] = jnp.where(sub == j, 1.0, -ratio)
        scale = 1.0 / jnp.sqrt(pivots)
        inside = (lane >= start) & (lane < stop)
        lead = jnp.where(inside, jnp.where(lane - start == sub, 1.0, 0.0), block)
        rows = columns[0] * spread(lead, 0)
        for k in range(1, width):
            rows = rows + columns[k] * spread(lead, k)
        rows = rows * scale
        out_ref[start:stop, :] = rows
        if stop < size:
            trail = jnp.where(lane >= stop, rows, 0.0)
            change = lax.dot_general(trail, rows, (((0,), (0,)), ((), ())), precision=HI, preferred_element_type=jnp.float32)
            rest = out_ref[stop:, :]
            hit = (column[stop:] >= start) & (column[stop:] < stop)
            out_ref[stop:, :] = jnp.where(hit, 0.0, rest) - change[stop:]
    if last == size:
        out_ref[...] = jnp.where(row >= column, out_ref[...], 0.0)


def inverse_factor(gram, pieces=2, width=16):
    size = gram.shape[0]
    state = gram
    for piece in range(pieces):
        first, last = size * piece // pieces, size * (piece + 1) // pieces
        call = pl.pallas_call(
            functools.partial(inverse_factor_body, first, last, width),
            out_shape=jax.ShapeDtypeStruct(gram.shape, jnp.float32),
            in_specs=[pl.BlockSpec(memory_space=pltpu.VMEM)],
            out_specs=pl.BlockSpec(memory_space=pltpu.VMEM),
            compiler_params=grant(2),
            cost_estimate=cost(3),
        )
        state = call(state)
    return state


def vmem(count):
    return [pl.BlockSpec(memory_space=pltpu.VMEM)] * count


SMEM = pl.BlockSpec(memory_space=pltpu.SMEM)


def grant(mebibytes, **more):
    return pltpu.CompilerParams(vmem_limit_bytes=mebibytes << 20, **more)


def cost(microseconds):
    return pl.CostEstimate(flops=int(microseconds * 1e9), bytes_accessed=1 << 17, transcendentals=0)


def terms_in_kernel(value, count):
    terms = []
    for _ in range(count):
        top = value.astype(jnp.bfloat16)
        terms.append(top)
        value = value - top.astype(jnp.float32)
    return terms


def exact_dot(narrow, wide, contract):
    dims = ((contract[:1], contract[1:]), ((), ()))
    total = None
    for term in reversed(terms_in_kernel(wide, 3)):
        part = lax.dot_general(narrow, term, dims, preferred_element_type=jnp.float32)
        total = part if total is None else total + part
    return total


def nt_dot(left, right):
    dims = (((1,), (1,)), ((), ()))
    return lax.dot_general(left, right, dims, precision=HI, preferred_element_type=jnp.float32)


def project_body(grads_ref, right_ref, out_ref, grads, right, arrived):
    depth = right_ref.shape[0]
    step = depth // 4 if depth % 512 == 0 else depth
    starts = range(0, depth, step)
    whole = pltpu.make_async_copy(grads_ref, grads, arrived.at[0])
    whole.start()
    copies = []
    for index, start in enumerate(starts):
        rows = pl.ds(start, step)
        copies.append(pltpu.make_async_copy(right_ref.at[rows, :], right.at[rows, :], arrived.at[1 + index]))
        copies[-1].start()
    whole.wait()
    total = None
    for copy, start in zip(copies, starts):
        copy.wait()
        part = exact_dot(grads[:, start : start + step], right[start : start + step, :], (1, 0))
        total = part if total is None else total + part
    out_ref[...] = total


def project(out_grads, right_prev):
    return pl.pallas_call(
        project_body,
        out_shape=jax.ShapeDtypeStruct((out_grads.shape[0], right_prev.shape[1]), jnp.float32),
        in_specs=[pl.BlockSpec(memory_space=pltpu.HBM)] * 2,
        out_specs=vmem(1)[0],
        scratch_shapes=[
            pltpu.VMEM(out_grads.shape, out_grads.dtype),
            pltpu.VMEM(right_prev.shape, right_prev.dtype),
            pltpu.SemaphoreType.DMA((5,)),
        ],
        compiler_params=grant(6),
        name="project",
    )(*(pltpu.with_memory_space_constraint(array, pltpu.HBM) for array in (out_grads, right_prev)))


def apply_body(place_ref, tall_ref, *refs):
    total = refs[0][...]
    for ref in refs[1:-1]:
        total = total + ref[...]
    rows = refs[-1].shape[0]
    mine = pl.ds(pl.multiple_of(place_ref[0] * rows, rows), rows)
    refs[-1][...] = exact_dot(tall_ref[mine, :], total, (1, 0))


def apply(place, tall, rows, parts):
    return pl.pallas_call(
        apply_body,
        out_shape=jax.ShapeDtypeStruct((rows, parts[0].shape[1]), jnp.float32),
        in_specs=[SMEM] + vmem(1 + len(parts)),
        out_specs=vmem(1)[0],
        compiler_params=grant(4),
        name="apply",
    )(place, tall, *parts)


def weigh_body(place_ref, tall_ref, left_ref, out_ref):
    rows = left_ref.shape[0]
    mine = pl.ds(pl.multiple_of(place_ref[0] * rows, rows), rows)
    out_ref[...] = exact_dot(tall_ref[mine, :], left_ref[...], (0, 0))


def weigh(place, tall, left):
    return pl.pallas_call(
        weigh_body,
        out_shape=jax.ShapeDtypeStruct((tall.shape[1], left.shape[1]), jnp.float32),
        in_specs=[SMEM] + vmem(2),
        out_specs=vmem(1)[0],
        compiler_params=grant(4),
        name="weigh",
    )(place, tall, left)


def basis_body(place_ref, inverse_ref, acts_ref, *refs):
    out_ref, rank = refs[-1], inverse_ref.shape[0]
    tokens = acts_ref.shape[1]
    out_ref[:, :tokens] = acts_ref[...]
    for part, ref in enumerate(refs[:-1]):
        rows = ref.shape[0]
        top, low = terms_in_kernel(-nt_dot(ref[...], inverse_ref[...]), 2)
        where = pl.ds(pl.multiple_of(place_ref[part] * rows, rows), rows)
        for index, term in enumerate((top, low, top)):
            out_ref[where, tokens + index * rank : tokens + (index + 1) * rank] = term


def basis(places, inverse, acts, parts):
    columns = acts.shape[1] + 3 * inverse.shape[0]
    return pl.pallas_call(
        basis_body,
        out_shape=jax.ShapeDtypeStruct((acts.shape[0], columns), jnp.bfloat16),
        in_specs=[SMEM] + vmem(2 + len(parts)),
        out_specs=vmem(1)[0],
        compiler_params=grant(8),
        cost_estimate=cost(2),
        name="basis",
    )(places, inverse, acts, *parts)


def blocks_fit(columns, axis):
    blocks = blocks_of(axis)
    return columns % blocks == 0 and columns // blocks % 128 == 0


def turn_body(replicas, inverse_ref, *refs):
    total = refs[0][...]
    for ref in refs[1:-1]:
        total = total + ref[...]
    right = nt_dot(total, inverse_ref[...]) * (1.0 / replicas)
    refs[-1][...] = jnp.transpose(right)


def turn(replicas, inverse, parts):
    rows, rank = parts[0].shape
    return pl.pallas_call(
        functools.partial(turn_body, replicas),
        out_shape=jax.ShapeDtypeStruct((rank, rows), jnp.float32),
        in_specs=vmem(1 + len(parts)),
        out_specs=vmem(1)[0],
        compiler_params=grant(2),
        name="turn",
    )(inverse, *parts)


def finish_body(replicas, turned, place_ref, mine_ref, tall_ref, grads_ref, sum_ref, inverse_ref, update_ref, residual_ref,
                wide, tiles, update, sent):
    tokens, rank = grads_ref.shape[0], inverse_ref.shape[0]
    count, tile = tiles.shape[:2]
    wide[:tokens, :] = grads_ref[...]
    width = sum_ref.shape[1] if turned else wide.shape[1]
    for start in range(0, wide.shape[1], width):
        if turned:
            first = start // width * rank
            top, low = terms_in_kernel(sum_ref[first : first + rank, :], 2)
        else:
            right = nt_dot(sum_ref[...], inverse_ref[...]) * (1.0 / replicas)
            top, low = (jnp.transpose(term) for term in terms_in_kernel(right, 2))
        for index, term in enumerate((top, top, low)):
            wide[tokens + index * rank : tokens + (index + 1) * rank, start : start + width] = term
    copies = []
    for index in range(count):
        rows = pl.ds(index * tile, tile)
        residual = jnp.dot(tall_ref[rows, :], wide[...], preferred_element_type=jnp.float32)
        tiles[index] = residual.astype(jnp.bfloat16)
        copies.append(pltpu.make_async_copy(tiles.at[index], residual_ref.at[rows, :], sent.at[index]))
        copies[-1].start()
        if index == 0:
            my_rows = update_ref.shape[0]
            mine = pl.ds(pl.multiple_of(place_ref[0] * my_rows, 16), my_rows)
            left = mine_ref[mine, tokens:] if my_rows % 16 == 0 else mine_ref[:, tokens:]
            update[...] = -jnp.dot(left, wide[tokens:, :], preferred_element_type=jnp.float32)
            copies.append(pltpu.make_async_copy(update, update_ref, sent.at[count]))
            copies[-1].start()
    for copy in copies:
        copy.wait()


def finish(replicas, turned, place, tall, out_grads, right_sum, inverse):
    rows, columns = tall.shape[0], out_grads.shape[1]
    my_rows, mine = rows // replicas, tall
    if my_rows % 16 != 0:
        mine = lax.dynamic_slice_in_dim(tall, place[0] * my_rows, my_rows, 0)
    tile = next(size for size in (256, 192, 128, 96, 64, 32, 16) if rows % size == 0)
    hbm = pl.BlockSpec(memory_space=pltpu.HBM)
    return pl.pallas_call(
        functools.partial(finish_body, replicas, turned),
        out_shape=(
            jax.ShapeDtypeStruct((my_rows, columns), jnp.float32),
            jax.ShapeDtypeStruct((rows, columns), jnp.bfloat16),
        ),
        in_specs=[SMEM] + vmem(5),
        out_specs=(hbm, hbm),
        scratch_shapes=[
            pltpu.VMEM((tall.shape[1], columns), jnp.bfloat16),
            pltpu.VMEM((rows // tile, tile, columns), jnp.bfloat16),
            pltpu.VMEM((my_rows, columns), jnp.float32),
            pltpu.SemaphoreType.DMA((rows // tile + 1,)),
        ],
        compiler_params=grant(20),
        name="finish",
    )(place, mine, tall, out_grads, right_sum, inverse)


def sent_all(value, axis):
    size, me = lax.axis_size(axis), lax.axis_index(axis)
    values, places = [value], [me]
    for step in range(1, size):
        values.append(shifted(value, axis, size, 1, step))
        places.append(source(me, step, size))
    return values, jnp.stack(places).astype(jnp.int32)


def per_device(activations, out_grads, right_prev):
    replicas, columns = lax.axis_size("dp"), lax.axis_size("tp")
    rows, my_columns = activations.shape[1], out_grads.shape[1]
    my_rows = rows // columns
    place = lax.axis_index("tp").astype(jnp.int32).reshape(1)
    origin = jnp.zeros((1,), jnp.int32)
    acts = lax.optimization_barrier(activations.T)

    projected, _ = sent_all(project(out_grads, right_prev), "tp")
    left_part = padded_rows(apply(place, acts, my_rows, projected), blocks_of("dp"))
    grads_late, left_part = lax.optimization_barrier((out_grads, left_part))
    grads = lax.optimization_barrier(grads_late.T)
    left_parts, _ = scatter_sum(left_part, "dp")
    left_own = gather_rows(together(left_parts, "dp"), "dp")[:my_rows]

    weighted_own, left_own = lax.optimization_barrier((weigh(place, acts, left_own), left_own))
    weighted, _ = sent_all(weighted_own, "tp")
    gram = jnp.dot(left_own.T, left_own, precision=HI)
    grams, _ = sent_all(gram, "tp")
    left_own, weighted[0] = lax.optimization_barrier((left_own, weighted[0]))
    right_part = apply(origin, grads, my_columns, weighted)
    right_part = padded_rows(right_part, blocks_of("dp"))
    right_parts, grams = scatter_sum(right_part, "dp", tied=grams)
    gram = sum(grams[1:], grams[0])

    parts, places = sent_all(left_own, "tp")
    inverse = inverse_factor(gram)
    turned = blocks_fit(my_columns, "dp") and len(right_parts) == 2
    right_own = turn(replicas, inverse, right_parts) if turned else together(right_parts, "dp")
    right_sum = gather_rows(right_own, "dp")
    right_sum = right_sum if turned else right_sum[:my_columns]
    tall = basis(places, inverse, acts, parts)
    replica = lax.axis_index("dp").astype(jnp.int32).reshape(1)
    return finish(replicas, turned, replica, tall, out_grads, right_sum, inverse)


def solution(mesh):
    in_specs = (P("dp", None), P("dp", "tp"), P("tp", None))
    out_specs = (P("dp", "tp"), P("dp", "tp"))
    return jax.shard_map(per_device, mesh=mesh, in_specs=in_specs, out_specs=out_specs, check_vma=False)
```
